32 devices in a mesh: ctx: 8 (over z, y), req: 4 (over x, core).
Axes of the slice: x: 2, y: 2, z: 4, core: 2. Of those that a mesh axis runs over, the one named last changes fastest.
Arguments:
- queries: bfloat16 [4096, 1024], P(('req', 'ctx')), parts along dimension 0, may hold values from -6 to 6
- keys: bfloat16 [4096, 256], P(('req', 'ctx')), parts along dimension 0, may hold values from -6 to 6
- lse: float32 [16, 4096], P(None, ('req', 'ctx')), parts along dimension 1, may hold values from -0.5 to 15, as said below
- length: int32 [4], P('req'), parts along dimension 0, may hold values from 512 to 1024
Outputs:
- key_scores: float32 [16, 4096], P(None, ('req', 'ctx')), parts along dimension 1
The draws below stay inside these ranges and needn't reach their ends.
There are 4 independent parts, one for each index of `req`. The reference program is written for one: setup_inputs(seed, part) draws one part's arguments, and reference() takes and returns one part's arrays. A program takes and returns all parts, laid end to end along the dimension named above; each array names one. Nothing has to cross between parts.
Inputs may be any that keep to these rules, and one draw needn't show every extreme that they name: lse[h, i] is the logarithm of i + 1 plus an offset between -0.5 and 3.
All inputs are finite; a program needn't handle non-finite values.
Results may differ from the reference program's by a relative error of at most 0.0003.
Values may be sent and summed in bfloat16 or wider, within the bound.
No kernel may reach another device: no remote copies, remote signals or barrier semaphores. Data moves between devices by JAX's collectives and lax.ppermute only.
A program may use at most 64 MiB of HBM per device.

```python
import math
import jax
import jax.numpy as jnp
from jax import lax

HEADS = 16
KV_HEADS = 4
HEAD_DIM = 64
TOKENS = 1024


def draw_lse(key, part):
    position = jnp.arange(TOKENS, dtype=jnp.float32)
    offset = jax.random.uniform(key, (HEADS, TOKENS), jnp.float32, 0.0, 2.0)
    return jnp.log(position + 1.0)[None, :] + offset


def steps_of(own_key, dims, cuts, low, high):
    level, own = 1.0, jax.random.fold_in(own_key, 6)
    for axis_at, parts in cuts:
        steps = jnp.exp(jax.random.uniform(jax.random.fold_in(own, axis_at), (parts,), jnp.float32, low / len(cuts), high / len(cuts)))
        level = level * jnp.repeat(steps, dims[axis_at] // parts).reshape([-1 if axis == axis_at else 1 for axis in range(len(dims))])
    return level


def centred(rng, shape, spread, most, cuts=(), kind=jnp.bfloat16):
    entries = spread * jax.random.normal(rng, shape, jnp.float32)
    if cuts:
        entries = entries * steps_of(rng, shape, cuts, -0.22, 0.18)
    return jnp.clip(entries, -most, most).astype(kind)


def setup_inputs(seed: int = 0, part: int = 0) -> dict:
    arg_keys = jax.random.split(jax.random.key(seed), 5)
    own_keys = jax.random.split(jax.random.fold_in(arg_keys[4], part), 5)
    return {
        "queries": centred(own_keys[0], (TOKENS, HEADS * HEAD_DIM), 1.0, 6.0, ((0, 8),)),
        "keys": centred(own_keys[1], (TOKENS, KV_HEADS * HEAD_DIM), 1.0, 6.0, ((0, 8),)),
        "lse": draw_lse(jax.random.fold_in(jax.random.fold_in(arg_keys[4], part), 71), part),
        "length": jax.random.randint(own_keys[3], (1,), TOKENS // 2, TOKENS + 1).astype(jnp.int32),
    }


def reference(queries, keys, lse, length):
    limit = length[0]
    positions = jnp.arange(TOKENS, dtype=jnp.int32)
    block_len = math.gcd(TOKENS, 256)
    group = HEADS // KV_HEADS
    grouped = queries.astype(jnp.float32).reshape(TOKENS, KV_HEADS, group, HEAD_DIM)

    def one_block(index):
        key_start = (index * block_len).astype(jnp.int32)
        key_block = lax.dynamic_slice_in_dim(keys, key_start, block_len, 0)
        key_view = key_block.astype(jnp.float32).reshape(block_len, KV_HEADS, HEAD_DIM)
        logits = jnp.einsum("rhgd,chd->hgrc", grouped, key_view).reshape(HEADS, TOKENS, block_len) * (HEAD_DIM ** -0.5)
        key_pos = key_start + jnp.arange(block_len, dtype=jnp.int32)
        valid = (positions[:, None] >= key_pos[None, :]) & (positions[:, None] < limit)
        weights = jnp.where(valid[None], jnp.exp(logits - lse[:, :, None]), jnp.float32(0.0))
        return jnp.sum(weights, axis=1)

    blocks = lax.map(one_block, jnp.arange(TOKENS // block_len, dtype=jnp.int32))
    return jnp.transpose(blocks, (1, 0, 2)).reshape(HEADS, TOKENS)
```

```python
import math

import jax
import jax.numpy as jnp
from jax import lax
from jax.experimental import pallas as pl
from jax.experimental.pallas import tpu as pltpu
from jax.sharding import PartitionSpec as P

HEAD_DIM = 64
LANES = 128
LOG2E = 1.4426950408889634
MASKED = 1e30
VMEM_BYTES = 8 * 1024 * 1024


def mass_kernel(pairs, query_xors, key_xors, has_init, length_ref, *refs):
    n_q, n_k = len(query_xors), len(key_xors)
    query_refs, refs = refs[:n_q], refs[n_q:]
    lse_refs, refs = refs[:n_q], refs[n_q:]
    key_refs, refs = refs[:n_k], refs[n_k:]
    init_ref = refs[0] if has_init else None
    out_ref = refs[-1]
    heads, rows = lse_refs[0].shape
    width = key_refs[0].shape[0]
    kv_heads = key_refs[0].shape[1] // HEAD_DIM
    group = heads // kv_heads
    me = lax.axis_index("ctx")
    limit = length_ref[0]
    scale = HEAD_DIM ** (-0.5) * LOG2E

    offsets = []
    for query_xor, lse_ref in zip(query_xors, lse_refs):
        row = (me ^ query_xor) * rows + lax.broadcasted_iota(jnp.int32, (heads, rows), 1)
        offsets.append(jnp.where(row < limit, lse_ref[...] * LOG2E, MASKED).T)
    low = lax.broadcasted_iota(jnp.int32, (width, LANES), 1) < HEAD_DIM
    causal = lax.broadcasted_iota(jnp.int32, (rows, width), 0) >= lax.broadcasted_iota(jnp.int32, (rows, width), 1)

    def block(j, chosen):
        key_ref = key_refs[j]
        for tile in range(key_ref.shape[1] // LANES):
            straight = key_ref[:, tile * LANES : (tile + 1) * LANES].astype(jnp.float32)
            swapped = pltpu.roll(straight, HEAD_DIM, 1)
            for half in range(LANES // HEAD_DIM):
                left, right = (straight, swapped) if half == 0 else (swapped, straight)
                spread = jnp.concatenate(
                    [jnp.where(low, left, 0.0), jnp.where(low, 0.0, right)], axis=0
                ).astype(jnp.bfloat16)
                first_head = (2 * tile + half) * group
                for head in range(first_head, first_head + group, 2):
                    lanes = slice(head * HEAD_DIM, (head + 2) * HEAD_DIM)
                    sums = [0.0, 0.0]
                    for i, diagonal in chosen:
                        logits = lax.dot_general(
                            query_refs[i][:, lanes],
                            spread,
                            (((1,), (1,)), ((), ())),
                            preferred_element_type=jnp.float32,
                        )
                        for side in range(2):
                            part = logits[:, side * width : (side + 1) * width]
                            weights = jnp.exp2(part * scale - offsets[i][:, head + side : head + side + 1])
                            if diagonal:
                                weights = jnp.where(causal, weights, 0.0)
                            sums[side] += jnp.sum(weights, axis=0, keepdims=True)
                    for side in range(2):
                        at = slice(j * heads + head + side, j * heads + head + side + 1)
                        out_ref[at, :] += sums[side]

    out_ref[...] = init_ref[...] if has_init else jnp.zeros_like(out_ref)
    for j, chosen in enumerate(pairs):
        always = [(i, True) for i in chosen if query_xors[i] == key_xors[j]]
        if always:
            block(j, always)
        later = [(i, False) for i in chosen if query_xors[i] != key_xors[j]]
        if later:
            first = query_xors[later[0][0]]

            @pl.when((me ^ first) > (me ^ key_xors[j]))
            def _():
                block(j, later)


def mass(pairs, query_sets, key_sets, length, init=None, name=None):
    heads, rows = query_sets[0][2].shape
    width = key_sets[0][1].shape[0]
    operands = [length]
    operands += [q for _, q, _ in query_sets] + [l for _, _, l in query_sets] + [k for _, k in key_sets]
    if init is not None:
        operands.append(init)
    n_pairs = sum(len(chosen) for chosen in pairs)
    body = lambda *refs: mass_kernel(
        pairs, [x for x, _, _ in query_sets], [x for x, _ in key_sets], init is not None, *refs
    )
    vmem = pl.BlockSpec(memory_space=pltpu.VMEM)
    return pl.pallas_call(
        body,
        out_shape=jax.ShapeDtypeStruct((len(key_sets) * heads, width), jnp.float32),
        in_specs=[pl.BlockSpec(memory_space=pltpu.SMEM)] + [vmem] * (len(operands) - 1),
        out_specs=vmem,
        cost_estimate=pl.CostEstimate(
            flops=2 * n_pairs * heads * rows * width * HEAD_DIM,
            bytes_accessed=sum(x.size * x.dtype.itemsize for x in operands),
            transcendentals=n_pairs * heads * rows * width,
        ),
        compiler_params=pltpu.CompilerParams(vmem_limit_bytes=VMEM_BYTES),
        name=name,
    )(*operands)


def swap_shards(queries, keys, lse, length):
    devices_ctx = lax.axis_size("ctx")
    heads = lse.shape[0]

    def swap(x, bit):
        return lax.ppermute(x, "ctx", [(i, i ^ bit) for i in range(devices_ctx)])

    lse_1 = swap(lse, 1)
    queries_1 = swap(queries, 1)
    keys_4 = swap(keys, 4)
    keys_6 = swap(keys, 6)
    keys_2 = swap(keys, 2)
    own = (0, queries, lse)
    partner = (1, queries_1, lse_1)
    near = mass([[0], [0]], [own], [(0, keys), (2, keys_2)], length, name="near_own")
    far = mass([[0], [0]], [own], [(4, keys_4), (6, keys_6)], length, name="far_own")
    far = mass([[0], [0]], [partner], [(4, keys_4), (6, keys_6)], length, far, name="far_partner")
    far_in = swap(far, 4)
    near = mass([[0], [0]], [partner], [(0, keys), (2, keys_2)], length, near, name="near_partner")
    near_in = swap(near[heads:] + far_in[heads:], 2)
    return near[:heads] + far_in[:heads] + near_in


def solution(mesh):
    placed = (P(("req", "ctx"), None), P(("req", "ctx"), None), P(None, ("req", "ctx")), P("req"))
    return jax.shard_map(
        swap_shards, mesh=mesh, in_specs=placed, out_specs=P(None, ("req", "ctx")), check_vma=False
    )
```

```python
import functools

import jax
import jax.numpy as jnp
from jax import lax
from jax.experimental import pallas as pl
from jax.experimental.pallas import tpu as pltpu
from jax.sharding import PartitionSpec as P


HEAD_DIM = 64
LANES = 128
LOG2E = 1.4426950408889634
MASKED = 1e30
VMEM_BYTES = 12 * 1024 * 1024


def spread_offsets(lse_ref, offset_ref, block_index, limit):
    heads, rows = lse_ref.shape
    row = block_index * rows + lax.broadcasted_iota(jnp.int32, (heads, rows), 1)
    columns = jnp.where(row < limit, lse_ref[...] * LOG2E, MASKED).T
    for head in range(heads):
        offset_ref[head] = jnp.broadcast_to(columns[:, head : head + 1], offset_ref.shape[1:])


def add_block(key_ref, query_refs, offset_refs, out_ref, diagonal=False):
    width = key_ref.shape[0]
    heads = out_ref.shape[0]
    group = heads * HEAD_DIM // key_ref.shape[1]
    scale = HEAD_DIM ** (-0.5) * LOG2E
    low = lax.broadcasted_iota(jnp.int32, (width, LANES), 1) < HEAD_DIM
    if diagonal:
        rows = query_refs[0].shape[0]
        causal = lax.broadcasted_iota(jnp.int32, (rows, width), 0) >= lax.broadcasted_iota(jnp.int32, (rows, width), 1)
    for tile in range(key_ref.shape[1] // LANES):
        straight = key_ref[:, tile * LANES : (tile + 1) * LANES].astype(jnp.float32)
        swapped = pltpu.roll(straight, HEAD_DIM, 1)
        for half in range(LANES // HEAD_DIM):
            left, right = (straight, swapped) if half == 0 else (swapped, straight)
            spread = jnp.concatenate([jnp.where(low, left, 0.0), jnp.where(low, 0.0, right)], axis=0)
            spread = spread.astype(jnp.bfloat16)
            first_head = (2 * tile + half) * group
            for head in range(first_head, first_head + group, 2):
                lanes = slice(head * HEAD_DIM, (head + 2) * HEAD_DIM)
                sums = [0.0, 0.0]
                for query_ref, offset_ref in zip(query_refs, offset_refs):
                    logits = lax.dot_general(
                        query_ref[:, lanes], spread, (((1,), (1,)), ((), ())), preferred_element_type=jnp.float32
                    )
                    for side in range(2):
                        part = logits[:, side * width : (side + 1) * width]
                        weights = jnp.exp2(part * scale - offset_ref[head + side])
                        if diagonal:
                            weights = jnp.where(causal, weights, 0.0)
                        sums[side] += jnp.sum(weights, axis=0, keepdims=True)
                for side in range(2):
                    out_ref[head + side : head + side + 1, :] += sums[side]


def local_kernel(length_ref, lse_hbm, query_hbm, key_hbm, lse_1_ref, own_ref, offset_ref, offset_1_ref, query_ref, key_ref, lse_ref, sems):
    copies = [
        pltpu.make_async_copy(source, target, sems.at[at])
        for at, (source, target) in enumerate([(lse_hbm, lse_ref), (key_hbm, key_ref), (query_hbm, query_ref)])
    ]
    for copy in copies:
        copy.start()
    me = lax.axis_index("ctx")
    limit = length_ref[0]
    spread_offsets(lse_1_ref, offset_1_ref, me ^ 1, limit)
    copies[0].wait()
    spread_offsets(lse_ref, offset_ref, me, limit)
    own_ref[...] = jnp.zeros_like(own_ref)
    copies[1].wait()
    copies[2].wait()
    add_block(key_ref, [query_ref], [offset_ref], own_ref, diagonal=True)


def pair_kernel(xor, query_ref, query_1_ref, offset_ref, offset_1_ref, key_ref, out_ref):
    me = lax.axis_index("ctx")
    out_ref[...] = jnp.zeros_like(out_ref)

    @pl.when((me ^ xor) < me)
    def _():
        add_block(key_ref, [query_ref, query_1_ref], [offset_ref, offset_1_ref], out_ref)


def near_kernel(xor, query_ref, query_1_ref, offset_ref, offset_1_ref, key_x_ref, own_in_ref, key_ref, out_ref, own_ref):
    me = lax.axis_index("ctx")
    pair_kernel(xor, query_ref, query_1_ref, offset_ref, offset_1_ref, key_x_ref, out_ref)
    own_ref[...] = own_in_ref[...]

    @pl.when((me ^ 1) > me)
    def _():
        add_block(key_ref, [query_1_ref], [offset_1_ref], own_ref)


def call(body, out_shapes, operands, pairs, in_specs=None, scratch=()):
    heads, rows, width = out_shapes[0].shape[0], operands[-1].shape[0], LANES
    vmem = pl.BlockSpec(memory_space=pltpu.VMEM)
    return pl.pallas_call(
        body,
        out_shape=out_shapes,
        in_specs=in_specs or [vmem] * len(operands),
        out_specs=[vmem] * len(out_shapes),
        scratch_shapes=scratch,
        cost_estimate=pl.CostEstimate(
            flops=2 * pairs * heads * rows * width * HEAD_DIM,
            bytes_accessed=sum(x.size * x.dtype.itemsize for x in operands),
            transcendentals=pairs * heads * rows * width,
        ),
        compiler_params=pltpu.CompilerParams(vmem_limit_bytes=VMEM_BYTES),
    )(*operands)


def far_xors(devices_ctx):
    return list(range(devices_ctx - 2, 2, -2))


def shards(queries, keys, lse, length):
    devices_ctx = lax.axis_size("ctx")
    heads, rows = lse.shape
    sums = jax.ShapeDtypeStruct((heads, keys.shape[0]), jnp.float32)
    offsets = jax.ShapeDtypeStruct((heads, rows, LANES), jnp.float32)

    def swap(x, bit):
        return lax.ppermute(x, "ctx", [(i, i ^ bit) for i in range(devices_ctx)])

    xors = far_xors(devices_ctx)
    lse_1 = swap(lse, 1)
    queries_1 = swap(queries, 1)
    keys_x = {x: swap(keys, x) for x in xors + [2]}

    hbm, vmem, smem = (pl.BlockSpec(memory_space=space) for space in (pltpu.HBM, pltpu.VMEM, pltpu.SMEM))
    own, offset, offset_1, queries, keys = call(
        local_kernel,
        [sums, offsets, offsets, queries, keys],
        [length] + [pltpu.with_memory_space_constraint(x, pltpu.HBM) for x in (lse, queries, keys)] + [lse_1],
        1,
        [smem, hbm, hbm, hbm, vmem],
        [pltpu.VMEM(lse.shape, lse.dtype), pltpu.SemaphoreType.DMA((3,))],
    )
    both = [queries, queries_1, offset, offset_1]
    back = []
    for x in xors:
        (part,) = call(functools.partial(pair_kernel, x), [sums], both + [keys_x[x]], 2)
        back.append(swap(part, x))
    part, own = call(functools.partial(near_kernel, 2), [sums, sums], both + [keys_x[2], own, keys], 3)
    back.append(swap(part, 2))
    for term in back:
        own = own + term
    return own


def solution(mesh):
    placed = (P(("req", "ctx"), None), P(("req", "ctx"), None), P(None, ("req", "ctx")), P("req"))

    return jax.shard_map(shards, mesh=mesh, in_specs=placed, out_specs=P(None, ("req", "ctx")), check_vma=False)
```

```python
import functools

import jax
import jax.numpy as jnp
from jax import lax
from jax.experimental import pallas as pl
from jax.experimental.pallas import tpu as pltpu
from jax.sharding import PartitionSpec as P


HEAD_DIM = 64
LANES = 128
LOG2E = 1.4426950408889634
MASKED = 1e30
VMEM_BYTES = 12 * 1024 * 1024
PIECES = 3


def offset_tile(lse_ref, block_index, limit):
    heads, rows = lse_ref.shape
    row = block_index * rows + lax.broadcasted_iota(jnp.int32, (heads, rows), 1)
    rest = jnp.where(row < limit, lse_ref[...], MASKED)
    pieces = []
    for _ in range(PIECES):
        piece = rest.astype(jnp.bfloat16).astype(jnp.float32)
        pieces.append(piece)
        rest = rest - piece
    pieces.append(jnp.zeros((LANES - PIECES * heads, rows), jnp.float32))
    return jnp.concatenate(pieces, axis=0).T.astype(jnp.bfloat16)


def add_block(key_ref, query_refs, offset_refs, out_ref, diagonal=False):
    width = key_ref.shape[0]
    heads = out_ref.shape[0]
    group = heads * HEAD_DIM // key_ref.shape[1]
    scale = HEAD_DIM ** (-0.5) * LOG2E
    low = lax.broadcasted_iota(jnp.int32, (width, LANES), 1) < HEAD_DIM
    lane = lax.broadcasted_iota(jnp.int32, (1, LANES), 1)
    offsets = jnp.concatenate([ref[...] for ref in offset_refs], axis=0)
    if diagonal:
        rows = query_refs[0].shape[0]
        causal = lax.broadcasted_iota(jnp.int32, (rows, width), 0) >= lax.broadcasted_iota(jnp.int32, (rows, width), 1)

    def picked(head):
        hit = lane == head
        for piece in range(1, PIECES):
            hit |= lane == piece * heads + head
        return jnp.broadcast_to(jnp.where(hit, -(HEAD_DIM**0.5), 0.0).astype(jnp.bfloat16), (width, LANES))

    for tile in range(key_ref.shape[1] // LANES):
        straight = key_ref[:, tile * LANES : (tile + 1) * LANES].astype(jnp.float32)
        swapped = pltpu.roll(straight, HEAD_DIM, 1)
        for half in range(LANES // HEAD_DIM):
            left, right = (straight, swapped) if half == 0 else (swapped, straight)
            spread = [jnp.where(low, left, 0.0).astype(jnp.bfloat16), jnp.where(low, 0.0, right).astype(jnp.bfloat16)]
            first_head = (2 * tile + half) * group
            for head in range(first_head, first_head + group, 2):
                lanes = slice(head * HEAD_DIM, (head + 2) * HEAD_DIM)
                deep = jnp.concatenate([ref[:, lanes] for ref in query_refs], axis=0)
                logits = lax.dot_general(
                    jnp.concatenate([deep, offsets], axis=1),
                    jnp.concatenate(
                        [jnp.concatenate([spread[side], picked(head + side)], axis=1) for side in range(2)], axis=0
                    ),
                    (((1,), (1,)), ((), ())),
                    preferred_element_type=jnp.float32,
                )
                for side in range(2):
                    weights = jnp.exp2(logits[:, side * width : (side + 1) * width] * scale)
                    if diagonal:
                        weights = jnp.where(causal, weights, 0.0)
                    out_ref[head + side : head + side + 1, :] += jnp.sum(weights, axis=0, keepdims=True)


def local_kernel(length_ref, lse_hbm, query_hbm, key_hbm, own_ref, offset_ref, query_ref, key_ref, lse_ref, sems):
    copies = [
        pltpu.make_async_copy(source, target, sems.at[at])
        for at, (source, target) in enumerate([(lse_hbm, lse_ref), (key_hbm, key_ref), (query_hbm, query_ref)])
    ]
    for copy in copies:
        copy.start()
    copies[0].wait()
    offset_ref[...] = offset_tile(lse_ref, lax.axis_index("ctx"), length_ref[0])
    own_ref[...] = jnp.zeros_like(own_ref)
    copies[1].wait()
    copies[2].wait()
    add_block(key_ref, [query_ref], [offset_ref], own_ref, diagonal=True)


def pair_kernel(xor, query_ref, query_1_ref, offset_ref, offset_1_ref, key_ref, out_ref):
    me = lax.axis_index("ctx")
    out_ref[...] = jnp.zeros_like(out_ref)

    @pl.when((me ^ xor) < me)
    def _():
        add_block(key_ref, [query_ref, query_1_ref], [offset_ref, offset_1_ref], out_ref)


def first_kernel(xor, length_ref, query_ref, query_1_ref, offset_ref, lse_1_ref, key_ref, out_ref, offset_1_ref):
    offset_1_ref[...] = offset_tile(lse_1_ref, lax.axis_index("ctx") ^ 1, length_ref[0])
    pair_kernel(xor, query_ref, query_1_ref, offset_ref, offset_1_ref, key_ref, out_ref)


def near_kernel(xor, query_ref, query_1_ref, offset_ref, offset_1_ref, key_x_ref, own_in_ref, key_ref, out_ref, own_ref):
    me = lax.axis_index("ctx")
    pair_kernel(xor, query_ref, query_1_ref, offset_ref, offset_1_ref, key_x_ref, out_ref)
    own_ref[...] = own_in_ref[...]

    @pl.when((me ^ 1) > me)
    def _():
        add_block(key_ref, [query_1_ref], [offset_1_ref], own_ref)


def call(body, out_shapes, operands, pairs, in_specs=None, scratch=()):
    heads, rows, width = out_shapes[0].shape[0], operands[-1].shape[0], LANES
    vmem = pl.BlockSpec(memory_space=pltpu.VMEM)
    return pl.pallas_call(
        body,
        out_shape=out_shapes,
        in_specs=in_specs or [vmem] * len(operands),
        out_specs=[vmem] * len(out_shapes),
        scratch_shapes=scratch,
        cost_estimate=pl.CostEstimate(
            flops=2 * pairs * heads * rows * width * HEAD_DIM,
            bytes_accessed=sum(x.size * x.dtype.itemsize for x in operands),
            transcendentals=pairs * heads * rows * width,
        ),
        compiler_params=pltpu.CompilerParams(vmem_limit_bytes=VMEM_BYTES),
    )(*operands)


def far_xors(devices_ctx):
    return list(range(devices_ctx - 2, 2, -2))


def shards(queries, keys, lse, length):
    devices_ctx = lax.axis_size("ctx")
    heads, rows = lse.shape
    sums = jax.ShapeDtypeStruct((heads, keys.shape[0]), jnp.float32)
    offsets = jax.ShapeDtypeStruct((rows, LANES), jnp.bfloat16)

    def swap(x, bit):
        return lax.ppermute(x, "ctx", [(i, i ^ bit) for i in range(devices_ctx)])

    xors = far_xors(devices_ctx)
    lse_1 = swap(lse, 1)
    queries_1 = swap(queries, 1)
    keys_x = {x: swap(keys, x) for x in xors + [2]}

    hbm, vmem, smem = (pl.BlockSpec(memory_space=space) for space in (pltpu.HBM, pltpu.VMEM, pltpu.SMEM))
    own, offset, queries, keys = call(
        local_kernel,
        [sums, offsets, queries, keys],
        [length] + [pltpu.with_memory_space_constraint(x, pltpu.HBM) for x in (lse, queries, keys)],
        1,
        [smem, hbm, hbm, hbm],
        [pltpu.VMEM(lse.shape, lse.dtype), pltpu.SemaphoreType.DMA((3,))],
    )
    back = []
    for x in xors:
        if not back:
            part, offset_1 = call(
                functools.partial(first_kernel, x),
                [sums, offsets],
                [length, queries, queries_1, offset, lse_1, keys_x[x]],
                2,
                [smem] + [vmem] * 5,
            )
            both = [queries, queries_1, offset, offset_1]
        else:
            (part,) = call(functools.partial(pair_kernel, x), [sums], both + [keys_x[x]], 2)
        back.append(swap(part, x))
    part, own = call(functools.partial(near_kernel, 2), [sums, sums], both + [keys_x[2], own, keys], 3)
    back.append(swap(part, 2))
    for term in back:
        own = own + term
    return own


def solution(mesh):
    placed = (P(("req", "ctx"), None), P(("req", "ctx"), None), P(None, ("req", "ctx")), P("req"))

    return jax.shard_map(shards, mesh=mesh, in_specs=placed, out_specs=P(None, ("req", "ctx")), check_vma=False)
```

```python
import functools

import jax
import jax.numpy as jnp
from jax import lax
from jax.experimental import pallas as pl
from jax.experimental.pallas import tpu as pltpu
from jax.sharding import PartitionSpec as P


HEAD_DIM = 64
LANES = 128
LOG2E = 1.4426950408889634
MASKED = 1e30
VMEM_BYTES = 12 * 1024 * 1024
PIECES = 3


def offset_tile(lse_ref, block_index, limit):
    heads, rows = lse_ref.shape
    row = block_index * rows + lax.broadcasted_iota(jnp.int32, (heads, rows), 1)
    rest = jnp.where(row < limit, lse_ref[...], MASKED)
    pieces = []
    for _ in range(PIECES):
        piece = rest.astype(jnp.bfloat16).astype(jnp.float32)
        pieces.append(piece)
        rest = rest - piece
    pieces.append(jnp.zeros((LANES - PIECES * heads, rows), jnp.float32))
    return jnp.concatenate(pieces, axis=0).T.astype(jnp.bfloat16)


def add_block(key_ref, query_refs, offset_refs, out_ref, diagonal=False):
    width = key_ref.shape[0]
    heads = out_ref.shape[0]
    group = heads * HEAD_DIM // key_ref.shape[1]
    scale = HEAD_DIM ** (-0.5) * LOG2E
    low = lax.broadcasted_iota(jnp.int32, (width, LANES), 1) < HEAD_DIM
    lane = lax.broadcasted_iota(jnp.int32, (1, LANES), 1)
    offsets = jnp.concatenate([ref[...] for ref in offset_refs], axis=0)
    if diagonal:
        rows = query_refs[0].shape[0]
        causal = lax.broadcasted_iota(jnp.int32, (rows, width), 0) >= lax.broadcasted_iota(jnp.int32, (rows, width), 1)

    def picked(head):
        hit = lane == head
        for piece in range(1, PIECES):
            hit |= lane == piece * heads + head
        return jnp.broadcast_to(jnp.where(hit, -(HEAD_DIM**0.5), 0.0).astype(jnp.bfloat16), (width, LANES))

    for tile in range(key_ref.shape[1] // LANES):
        straight = key_ref[:, tile * LANES : (tile + 1) * LANES].astype(jnp.float32)
        swapped = pltpu.roll(straight, HEAD_DIM, 1)
        for half in range(LANES // HEAD_DIM):
            left, right = (straight, swapped) if half == 0 else (swapped, straight)
            spread = [jnp.where(low, left, 0.0).astype(jnp.bfloat16), jnp.where(low, 0.0, right).astype(jnp.bfloat16)]
            first_head = (2 * tile + half) * group
            for head in range(first_head, first_head + group, 2):
                lanes = slice(head * HEAD_DIM, (head + 2) * HEAD_DIM)
                deep = jnp.concatenate([ref[:, lanes] for ref in query_refs], axis=0)
                logits = lax.dot_general(
                    jnp.concatenate([deep, offsets], axis=1),
                    jnp.concatenate(
                        [jnp.concatenate([spread[side], picked(head + side)], axis=1) for side in range(2)], axis=0
                    ),
                    (((1,), (1,)), ((), ())),
                    preferred_element_type=jnp.float32,
                )
                for side in range(2):
                    weights = jnp.exp2(logits[:, side * width : (side + 1) * width] * scale)
                    if diagonal:
                        weights = jnp.where(causal, weights, 0.0)
                    out_ref[head + side : head + side + 1, :] += jnp.sum(weights, axis=0, keepdims=True)


def local_kernel(length_ref, lse_hbm, query_hbm, key_hbm, own_ref, offset_ref, query_ref, key_ref, lse_ref, sems):
    copies = [
        pltpu.make_async_copy(source, target, sems.at[at])
        for at, (source, target) in enumerate([(lse_hbm, lse_ref), (key_hbm, key_ref), (query_hbm, query_ref)])
    ]
    for copy in copies:
        copy.start()
    copies[0].wait()
    offset_ref[...] = offset_tile(lse_ref, lax.axis_index("ctx"), length_ref[0])
    own_ref[...] = jnp.zeros_like(own_ref)
    copies[1].wait()
    copies[2].wait()
    add_block(key_ref, [query_ref], [offset_ref], own_ref, diagonal=True)


def pair_kernel(xor, query_ref, query_1_ref, offset_ref, offset_1_ref, key_ref, out_ref):
    me = lax.axis_index("ctx")
    out_ref[...] = jnp.zeros_like(out_ref)

    @pl.when((me ^ xor) < me)
    def _():
        add_block(key_ref, [query_ref, query_1_ref], [offset_ref, offset_1_ref], out_ref)


def first_kernel(xor, length_ref, query_ref, query_1_ref, offset_ref, lse_1_ref, key_ref, out_ref, offset_1_ref):
    offset_1_ref[...] = offset_tile(lse_1_ref, lax.axis_index("ctx") ^ 1, length_ref[0])
    pair_kernel(xor, query_ref, query_1_ref, offset_ref, offset_1_ref, key_ref, out_ref)


def partner_kernel(query_1_ref, offset_1_ref, key_ref, own_in_ref, own_ref):
    me = lax.axis_index("ctx")
    own_ref[...] = own_in_ref[...]

    @pl.when((me ^ 1) > me)
    def _():
        add_block(key_ref, [query_1_ref], [offset_1_ref], own_ref)


def call(body, out_shapes, operands, pairs, in_specs=None, scratch=()):
    heads, rows, width = out_shapes[0].shape[0], operands[-1].shape[0], LANES
    vmem = pl.BlockSpec(memory_space=pltpu.VMEM)
    return pl.pallas_call(
        body,
        out_shape=out_shapes,
        in_specs=in_specs or [vmem] * len(operands),
        out_specs=[vmem] * len(out_shapes),
        scratch_shapes=scratch,
        cost_estimate=pl.CostEstimate(
            flops=2 * pairs * heads * rows * width * HEAD_DIM,
            bytes_accessed=sum(x.size * x.dtype.itemsize for x in operands),
            transcendentals=pairs * heads * rows * width,
        ),
        compiler_params=pltpu.CompilerParams(vmem_limit_bytes=VMEM_BYTES),
    )(*operands)


def far_xors(devices_ctx):
    return list(range(devices_ctx - 2, 2, -2))


def shards(queries, keys, lse, length):
    devices_ctx = lax.axis_size("ctx")
    heads, rows = lse.shape
    sums = jax.ShapeDtypeStruct((heads, keys.shape[0]), jnp.float32)
    offsets = jax.ShapeDtypeStruct((rows, LANES), jnp.bfloat16)

    def swap(x, bit, up=None):
        pairs = [(i, i ^ bit if up is None or i ^ bit < i else i ^ up) for i in range(devices_ctx)]
        return lax.ppermute(x, "ctx", pairs)

    xors = far_xors(devices_ctx)
    lse_1 = swap(lse, 1)
    queries_1 = swap(queries, 1)
    keys_x = {x: swap(keys, x) for x in xors + [2]}

    hbm, vmem, smem = (pl.BlockSpec(memory_space=space) for space in (pltpu.HBM, pltpu.VMEM, pltpu.SMEM))
    own, offset, queries, keys = call(
        local_kernel,
        [sums, offsets, queries, keys],
        [length] + [pltpu.with_memory_space_constraint(x, pltpu.HBM) for x in (lse, queries, keys)],
        1,
        [smem, hbm, hbm, hbm],
        [pltpu.VMEM(lse.shape, lse.dtype), pltpu.SemaphoreType.DMA((3,))],
    )
    back = []
    for x in xors:
        if not back:
            part, offset_1 = call(
                functools.partial(first_kernel, x),
                [sums, offsets],
                [length, queries, queries_1, offset, lse_1, keys_x[x]],
                2,
                [smem] + [vmem] * 5,
            )
            both = [queries, queries_1, offset, offset_1]
        else:
            (part,) = call(functools.partial(pair_kernel, x), [sums], both + [keys_x[x]], 2)
        back.append(swap(part, x, up=1 << (x.bit_length() - 1)))
    (part,) = call(functools.partial(pair_kernel, 2), [sums], both + [keys_x[2]], 2)
    back.append(swap(part, 2))
    (own,) = call(partner_kernel, [sums], [queries_1, offset_1, keys, own], 1)
    for term in back:
        own = own + term
    return own


def solution(mesh):
    placed = (P(("req", "ctx"), None), P(("req", "ctx"), None), P(None, ("req", "ctx")), P("req"))

    return jax.shard_map(shards, mesh=mesh, in_specs=placed, out_specs=P(None, ("req", "ctx")), check_vma=False)
```

```python
import functools

import jax
import jax.numpy as jnp
from jax import lax
from jax.experimental import pallas as pl
from jax.experimental.pallas import tpu as pltpu
from jax.sharding import PartitionSpec as P


HEAD_DIM = 64
LANES = 128
LOG2E = 1.4426950408889634
MASKED = 1e30
VMEM_BYTES = 12 * 1024 * 1024
PIECES = 3


def offset_tile(lse_ref, block_index, limit):
    heads, rows = lse_ref.shape
    row = block_index * rows + lax.broadcasted_iota(jnp.int32, (heads, rows), 1)
    rest = jnp.where(row < limit, lse_ref[...], MASKED)
    pieces = []
    for _ in range(PIECES):
        piece = rest.astype(jnp.bfloat16).astype(jnp.float32)
        pieces.append(piece)
        rest = rest - piece
    pieces.append(jnp.zeros((LANES - PIECES * heads, rows), jnp.float32))
    return jnp.concatenate(pieces, axis=0).T.astype(jnp.bfloat16)


def add_block(key_ref, query_refs, offset_refs, out_ref, diagonal=False):
    width = key_ref.shape[0]
    heads = out_ref.shape[0]
    group = heads * HEAD_DIM // key_ref.shape[1]
    scale = HEAD_DIM ** (-0.5) * LOG2E
    low = lax.broadcasted_iota(jnp.int32, (width, LANES), 1) < HEAD_DIM
    lane = lax.broadcasted_iota(jnp.int32, (1, LANES), 1)
    offsets = jnp.concatenate([ref[...] for ref in offset_refs], axis=0)
    if diagonal:
        rows = query_refs[0].shape[0]
        causal = lax.broadcasted_iota(jnp.int32, (rows, width), 0) >= lax.broadcasted_iota(jnp.int32, (rows, width), 1)

    def picked(head):
        hit = lane == head
        for piece in range(1, PIECES):
            hit |= lane == piece * heads + head
        return jnp.broadcast_to(jnp.where(hit, -(HEAD_DIM**0.5), 0.0).astype(jnp.bfloat16), (width, LANES))

    for tile in range(key_ref.shape[1] // LANES):
        straight = key_ref[:, tile * LANES : (tile + 1) * LANES].astype(jnp.float32)
        swapped = pltpu.roll(straight, HEAD_DIM, 1)
        for half in range(LANES // HEAD_DIM):
            left, right = (straight, swapped) if half == 0 else (swapped, straight)
            spread = [jnp.where(low, left, 0.0).astype(jnp.bfloat16), jnp.where(low, 0.0, right).astype(jnp.bfloat16)]
            first_head = (2 * tile + half) * group
            for head in range(first_head, first_head + group, 2):
                lanes = slice(head * HEAD_DIM, (head + 2) * HEAD_DIM)
                deep = jnp.concatenate([ref[:, lanes] for ref in query_refs], axis=0)
                logits = lax.dot_general(
                    jnp.concatenate([deep, offsets], axis=1),
                    jnp.concatenate(
                        [jnp.concatenate([spread[side], picked(head + side)], axis=1) for side in range(2)], axis=0
                    ),
                    (((1,), (1,)), ((), ())),
                    preferred_element_type=jnp.float32,
                )
                for side in range(2):
                    weights = jnp.exp2(logits[:, side * width : (side + 1) * width] * scale)
                    if diagonal:
                        weights = jnp.where(causal, weights, 0.0)
                    out_ref[head + side : head + side + 1, :] += jnp.sum(weights, axis=0, keepdims=True)


def local_kernel(length_ref, lse_hbm, query_hbm, key_hbm, own_ref, offset_ref, query_ref, key_ref, lse_ref, sems):
    copies = [
        pltpu.make_async_copy(source, target, sems.at[at])
        for at, (source, target) in enumerate([(lse_hbm, lse_ref), (key_hbm, key_ref), (query_hbm, query_ref)])
    ]
    for copy in copies:
        copy.start()
    copies[0].wait()
    offset_ref[...] = offset_tile(lse_ref, lax.axis_index("ctx"), length_ref[0])
    own_ref[...] = jnp.zeros_like(own_ref)
    copies[1].wait()
    copies[2].wait()
    add_block(key_ref, [query_ref], [offset_ref], own_ref, diagonal=True)


def pair_kernel(xor, query_ref, query_1_ref, offset_ref, offset_1_ref, key_ref, *refs, upper=None):
    out_ref = refs[-1]
    me = lax.axis_index("ctx")
    out_ref[...] = refs[0][...] if len(refs) > 1 else jnp.zeros_like(out_ref)
    wanted = (me ^ xor) < me
    if upper is not None:
        wanted &= (me >= lax.axis_size("ctx") // 2) == upper

    @pl.when(wanted)
    def _():
        add_block(key_ref, [query_ref, query_1_ref], [offset_ref, offset_1_ref], out_ref)


def first_kernel(xor, length_ref, query_ref, query_1_ref, offset_ref, lse_1_ref, key_ref, out_ref, offset_1_ref):
    offset_1_ref[...] = offset_tile(lse_1_ref, lax.axis_index("ctx") ^ 1, length_ref[0])
    pair_kernel(xor, query_ref, query_1_ref, offset_ref, offset_1_ref, key_ref, out_ref)


def partner_kernel(query_1_ref, offset_1_ref, key_ref, own_in_ref, own_ref):
    me = lax.axis_index("ctx")
    own_ref[...] = own_in_ref[...]

    @pl.when((me ^ 1) > me)
    def _():
        add_block(key_ref, [query_1_ref], [offset_1_ref], own_ref)


def call(body, out_shapes, operands, pairs, in_specs=None, scratch=()):
    heads, rows, width = out_shapes[0].shape[0], operands[-1].shape[0], LANES
    vmem = pl.BlockSpec(memory_space=pltpu.VMEM)
    return pl.pallas_call(
        body,
        out_shape=out_shapes,
        in_specs=in_specs or [vmem] * len(operands),
        out_specs=[vmem] * len(out_shapes),
        scratch_shapes=scratch,
        cost_estimate=pl.CostEstimate(
            flops=2 * pairs * heads * rows * width * HEAD_DIM,
            bytes_accessed=sum(x.size * x.dtype.itemsize for x in operands),
            transcendentals=pairs * heads * rows * width,
        ),
        compiler_params=pltpu.CompilerParams(vmem_limit_bytes=VMEM_BYTES),
    )(*operands)


def far_xors(devices_ctx):
    if devices_ctx < 8 or devices_ctx & (devices_ctx - 1):
        raise ValueError(devices_ctx)
    return list(range(devices_ctx - 2, 2, -2))


def shards(queries, keys, lse, length):
    devices_ctx = lax.axis_size("ctx")
    heads, rows = lse.shape
    sums = jax.ShapeDtypeStruct((heads, keys.shape[0]), jnp.float32)
    offsets = jax.ShapeDtypeStruct((rows, LANES), jnp.bfloat16)

    def swap(x, bit, up=None):
        pairs = [(i, i ^ bit if up is None or i ^ bit < i else i ^ up) for i in range(devices_ctx)]
        return lax.ppermute(x, "ctx", pairs)

    xors = far_xors(devices_ctx)
    lse_1 = swap(lse, 1)
    queries_1 = swap(queries, 1)
    keys_x = {x: swap(keys, x) for x in xors + [2]}

    hbm, vmem, smem = (pl.BlockSpec(memory_space=space) for space in (pltpu.HBM, pltpu.VMEM, pltpu.SMEM))
    own, offset, queries, keys = call(
        local_kernel,
        [sums, offsets, queries, keys],
        [length] + [pltpu.with_memory_space_constraint(x, pltpu.HBM) for x in (lse, queries, keys)],
        1,
        [smem, hbm, hbm, hbm],
        [pltpu.VMEM(lse.shape, lse.dtype), pltpu.SemaphoreType.DMA((3,))],
    )
    back = []
    for x in xors:
        if not back:
            part, offset_1 = call(
                functools.partial(first_kernel, x),
                [sums, offsets],
                [length, queries, queries_1, offset, lse_1, keys_x[x]],
                2,
                [smem] + [vmem] * 5,
            )
            both = [queries, queries_1, offset, offset_1]
        else:
            (part,) = call(functools.partial(pair_kernel, x), [sums], both + [keys_x[x]], 2)
        back.append(swap(part, x, up=1 << (x.bit_length() - 1)))
    near = both + [keys_x[2]]
    (part,) = call(functools.partial(pair_kernel, 2, upper=False), [sums], near, 2)
    (part,) = call(functools.partial(pair_kernel, 2, upper=True), [sums], near + [part], 2)
    back.append(swap(part, 2))
    (own,) = call(partner_kernel, [sums], [queries_1, offset_1, keys, own], 1)
    for term in back:
        own = own + term
    return own


def solution(mesh):
    placed = (P(("req", "ctx"), None), P(("req", "ctx"), None), P(None, ("req", "ctx")), P("req"))

    return jax.shard_map(shards, mesh=mesh, in_specs=placed, out_specs=P(None, ("req", "ctx")), check_vma=False)
```
